32 devices in a mesh: corpus: 16 (over z, y, x), tensor: 2 (over core).
Axes of the slice: x: 2, y: 2, z: 4, core: 2. Of those that a mesh axis runs over, the one named last changes fastest.
Arguments:
- q_states: bfloat16 [1024, 4096], P('corpus', 'tensor'), may hold values from -90 to 90
- k_states: bfloat16 [1024, 1024], P('corpus', 'tensor'), may hold values from -9 to 9
- v_states: bfloat16 [1024, 1024], P('corpus', 'tensor'), may hold values from -6 to 6
- residual: bfloat16 [1024, 4096], P('corpus'), may hold values from -170 to 170
- out_weight: bfloat16 [4096, 4096], P('tensor'), may hold values from -0.09375 to 0.09375
- final_gain: float32 [4096], replicated, may hold values from 0.25 to 1.75
- passages: bfloat16 [8192, 4096], P(('corpus', 'tensor')), may hold values from -5 to 5
- lengths: int32 [64], P('corpus'), may hold values from 1 to 16
Outputs:
- scores: float32 [64, 8192], P(None, ('corpus', 'tensor'))
- log_norm: float32 [64], replicated
The draws below stay inside these ranges and needn't reach their ends.
All inputs are finite; a program needn't handle non-finite values.
Results may differ from the reference program's by a relative error of at most 0.0003.
The reference program's roundings to bfloat16 on the way (of `weights`, `context` and `embed`) count: a program that leaves them out, or rounds other values in their place, can miss the bound.
Values may be sent and summed in bfloat16 or wider, within the bound.
A program may use at most 64 MiB of HBM per device.

```python
import math
import jax
import jax.numpy as jnp
from jax import lax

D = 4096
HEADS = 32
KV_HEADS = 8
HEAD_DIM = 128
SEQ = 16
QUERIES = 64
TOKENS = 1024
PASSAGES = 8192
Q_WIDTH = 4096
KV_WIDTH = 1024


def key_values(key):
    return jnp.clip(jax.random.normal(jax.random.fold_in(key, 2), (TOKENS, KV_HEADS * HEAD_DIM), jnp.float32), -6.0, 6.0)


def draw_k_states(key, part):
    drawn = key_values(key)
    return drawn.astype(jnp.bfloat16)


def draw_q_states(key, part):
    entries = jnp.clip(jax.random.normal(jax.random.fold_in(key, 3), (TOKENS, HEADS * HEAD_DIM), jnp.float32), -6.0, 6.0)
    return entries.astype(jnp.bfloat16)


def draw_residual(key, part):
    entries = jnp.clip(jax.random.normal(jax.random.fold_in(key, 1), (TOKENS, D), jnp.float32), -6.0, 6.0)
    return entries.astype(jnp.bfloat16)


def draw_passages(key, part):
    entries = jnp.clip(jax.random.normal(jax.random.fold_in(key, 5), (PASSAGES, D), jnp.float32), -6.0, 6.0) * 0.0625
    return entries.astype(jnp.bfloat16)


def plant(result, stream_key, least, high):
    place = [jax.random.randint(jax.random.fold_in(stream_key, axis), (), 0, length) for axis, length in enumerate(result.shape)]
    widest = result.shape.index(max(result.shape))
    neighbour = place[:widest] + [(place[widest] + 1) % result.shape[widest]] + place[widest + 1:]
    return result.at[tuple(place)].set(least).at[tuple(neighbour)].set(high)


def level_of(own_key, dims, shards, least, high):
    level = 1.0
    for position, blocks in shards:
        steps = jax.random.uniform(jax.random.fold_in(jax.random.fold_in(own_key, 6), position), (blocks,), jnp.float32, least / len(shards), high / len(shards))
        level = level * jnp.repeat(jnp.exp(steps), dims[position] // blocks).reshape((-1,) + (1,) * (len(dims) - 1 - position))
    return level


def bell_draw(stream_key, dims, scale, limit, cuts=(), held_as=jnp.bfloat16):
    gain = level_of(stream_key, dims, cuts, -0.22, 0.18) if cuts else 1.0
    values = jax.random.normal(stream_key, dims, jnp.float32) * scale * gain
    return jnp.minimum(jnp.maximum(values, -limit), limit).astype(held_as)


def setup_inputs(seed: int = 0) -> dict:
    arg_keys = jax.random.split(jax.random.key(seed), 9)
    return {
        "q_states": draw_q_states(jax.random.fold_in(arg_keys[8], 71), 0),
        "k_states": draw_k_states(jax.random.fold_in(arg_keys[8], 71), 0),
        "v_states": bell_draw(arg_keys[2], (TOKENS, KV_WIDTH), 1.0, 6.0, ((0, 16), (1, 2))),
        "residual": draw_residual(jax.random.fold_in(arg_keys[8], 71), 0),
        "out_weight": bell_draw(arg_keys[4], (Q_WIDTH, D), Q_WIDTH ** -0.5, 0.09375, ((0, 2),)),
        "final_gain": jnp.clip(1.0 + 0.15 * jax.random.normal(arg_keys[5], (D,), jnp.float32), 0.25, 1.75),
        "passages": draw_passages(jax.random.fold_in(arg_keys[8], 71), 0),
        "lengths": plant(jax.random.randint(arg_keys[7], (QUERIES,), 1, SEQ + 1), jax.random.fold_in(arg_keys[7], 1), 1, SEQ).astype(jnp.int32),
    }


score_scale = 50.0

def attend_rows(queries, key_rows, value_rows, query_place, lengths):
    query_count = queries.shape[0]
    query_span = queries.shape[1]
    pair_heads = key_rows.shape[2] // HEAD_DIM
    grouped = queries.astype(jnp.float32).reshape(query_count, query_span, pair_heads, -1, HEAD_DIM)
    keyed = key_rows.astype(jnp.float32).reshape(query_count, SEQ, pair_heads, HEAD_DIM)
    valued = value_rows.astype(jnp.float32).reshape(query_count, SEQ, pair_heads, HEAD_DIM)
    logits = jnp.einsum('brkgd,bskd->bkgrs', grouped, keyed) / math.sqrt(HEAD_DIM)
    key_place = lax.broadcasted_iota(jnp.int32, (1, 1, SEQ), 2)
    allowed = (key_place <= query_place[:, :, None]) & (key_place < lengths[:, None, None])
    allowed = allowed[:, None, None, :, :]
    logits = jnp.where(allowed, logits, -1e+30)
    highest = lax.optimization_barrier(jnp.max(logits, axis=-1, keepdims=True))
    weights = jnp.where(allowed, jnp.exp(logits - highest), 0.0)
    attention = (weights / lax.optimization_barrier(jnp.sum(weights, axis=-1, keepdims=True))).astype(jnp.bfloat16)
    context = jnp.einsum('bkgrs,bskd->brkgd', attention.astype(jnp.float32), valued)
    return context.reshape(query_count * query_span, -1).astype(jnp.bfloat16)

def reference(q_states, k_states, v_states, residual, out_weight, final_gain, passages, lengths):
    query_count = lengths.shape[0]
    places = lax.broadcasted_iota(jnp.int32, (query_count, SEQ), 1)
    context = attend_rows(q_states.reshape(query_count, SEQ, -1), k_states.reshape(query_count, SEQ, -1), v_states.reshape(query_count, SEQ, -1), places, lengths)
    attended = jnp.dot(context, out_weight, preferred_element_type=jnp.float32)
    hidden = residual.astype(jnp.float32) + attended
    picker = (places == (lengths - 1)[:, None]).astype(jnp.float32)
    pooled = lax.optimization_barrier(jnp.sum(picker[:, :, None] * hidden.reshape(query_count, SEQ, -1), axis=1))
    scaled = pooled * final_gain.astype(jnp.float32)[None, :]
    magnitude = jnp.maximum(jnp.sqrt(lax.optimization_barrier(jnp.sum(scaled * scaled, axis=1, keepdims=True))), 1.0)
    embed = (scaled / magnitude).astype(jnp.bfloat16)
    scores = jnp.dot(embed, passages.T, preferred_element_type=jnp.float32) * score_scale
    highest = lax.optimization_barrier(jnp.max(scores, axis=1))
    log_norm = highest + jnp.log(lax.optimization_barrier(jnp.sum(jnp.exp(scores - highest[:, None]), axis=1)))
    return (scores, log_norm)
```

```python
import math

import jax
import jax.numpy as jnp
from jax import lax
from jax.sharding import PartitionSpec as P

HEAD_DIM = 128
SEQ = 16


score_scale = 50.0


def merged(value, axis, join):
    pieces = jax.tree.map(lambda part: lax.all_gather(part, axis), value)
    head = jax.tree.map(lambda part: part[0], pieces)
    tail = jax.tree.map(lambda part: part[1:], pieces)
    total, _ = lax.scan(lambda total, piece: (join(total, piece), None), head, tail)
    return total


def attend_last(queries, key_rows, value_rows, lengths):
    query_count = queries.shape[0]
    pair_heads = key_rows.shape[2] // HEAD_DIM
    grouped = queries.reshape(query_count, pair_heads, -1, HEAD_DIM)
    keyed = key_rows.reshape(query_count, SEQ, pair_heads, HEAD_DIM)
    valued = value_rows.reshape(query_count, SEQ, pair_heads, HEAD_DIM)
    logits = jnp.einsum(
        "bkgd,bskd->bkgs", grouped, keyed, preferred_element_type=jnp.float32
    ) / math.sqrt(HEAD_DIM)
    key_place = lax.broadcasted_iota(jnp.int32, (1, SEQ), 1)
    allowed = (key_place < lengths[:, None])[:, None, None, :]
    logits = jnp.where(allowed, logits, -1e30)
    highest = jnp.max(logits, axis=-1, keepdims=True)
    weights = jnp.where(allowed, jnp.exp(logits - highest), 0.0)
    attention = (weights / jnp.sum(weights, axis=-1, keepdims=True)).astype(jnp.bfloat16)
    context = jnp.einsum("bkgs,bskd->bkgd", attention, valued, preferred_element_type=jnp.float32)
    return context.reshape(query_count, -1).astype(jnp.bfloat16)


def normalize_rows(pooled, final_gain):
    scaled = pooled * final_gain[None, :]
    magnitude = jnp.maximum(jnp.sqrt(jnp.sum(scaled * scaled, axis=1, keepdims=True)), 1.0)
    return (scaled / magnitude).astype(jnp.bfloat16)


def on_device(q_states, k_states, v_states, residual, out_weight, final_gain, passages, lengths):
    query_count = lengths.shape[0]
    places = lax.broadcasted_iota(jnp.int32, (query_count, SEQ), 1)
    picked = (places == (lengths - 1)[:, None])[:, :, None]
    key_rows = k_states.reshape(query_count, SEQ, -1)
    value_rows = v_states.reshape(query_count, SEQ, -1)
    last_query = jnp.sum(
        jnp.where(picked, q_states.reshape(query_count, SEQ, -1).astype(jnp.float32), 0.0), axis=1
    ).astype(jnp.bfloat16)
    last_residual = jnp.sum(
        jnp.where(picked, residual.reshape(query_count, SEQ, -1).astype(jnp.float32), 0.0), axis=1
    )
    context = attend_last(last_query, key_rows, value_rows, lengths)
    partial_value = jnp.dot(context, out_weight, preferred_element_type=jnp.float32)
    pooled = last_residual + lax.psum(partial_value, "tensor")
    embed = normalize_rows(pooled, final_gain)
    scores = (
        lax.dot_general(
            lax.all_gather(embed, "corpus", axis=0, tiled=True),
            passages,
            (((1,), (1,)), ((), ())),
            preferred_element_type=jnp.float32,
        )
        * score_scale
    )
    local_peak = jnp.max(scores, axis=1)
    local_total = jnp.sum(jnp.exp(scores - local_peak[:, None]), axis=1)

    def combine(former, latter):
        highest = jnp.maximum(former[0], latter[0])
        return (
            highest,
            former[1] * jnp.exp(former[0] - highest) + latter[1] * jnp.exp(latter[0] - highest),
        )

    global_peak, global_total = merged((local_peak, local_total), ("corpus", "tensor"), combine)
    return (scores, global_peak + jnp.log(global_total))


def solution(mesh):
    in_specs = (
        P("corpus", "tensor"),
        P("corpus", "tensor"),
        P("corpus", "tensor"),
        P("corpus", None),
        P("tensor", None),
        P(),
        P(("corpus", "tensor"), None),
        P("corpus"),
    )
    out_specs = (P(None, ("corpus", "tensor")), P())
    return jax.shard_map(
        on_device, mesh=mesh, in_specs=in_specs, out_specs=out_specs, check_vma=False
    )
```

```python
import functools
import math

import jax
import jax.numpy as jnp
from jax import lax
from jax.experimental import pallas as pl
from jax.experimental.pallas import tpu as pltpu
from jax.sharding import PartitionSpec as P

HEAD_DIM = 128
SEQ = 16
GROUP = 4
SCORE_SCALE = 50.0
F32 = jnp.float32
BF16 = jnp.bfloat16


def kernel(
    sizes, lengths, q_hbm, k_hbm, v_hbm, res_hbm, w_hbm, gain_hbm, pass_hbm,
    scores_hbm, norm_ref,
    q_ref, k_ref, v_ref, res_ref, w_ref, gain_ref, pass_ref,
    part, gathered, embed, scores_ref, pair_stat, all_stat,
    in_sem, w_sem, out_sem,
    part_send, part_recv, far_send, far_recv, near_send, near_recv, twin_send, twin_recv,
    pair_send, pair_recv, stat_send, stat_recv,
):
    corpus, tensor, group, chunks = sizes
    spans = corpus // group
    query_count = lengths.shape[0]
    rows = part.shape[2]
    key_count = k_ref.shape[0]
    kv_heads = k_ref.shape[1] // HEAD_DIM
    per_kv = q_ref.shape[1] // k_ref.shape[1]
    width = w_ref.shape[1]
    chunk = width // chunks
    share = width // tensor
    mine = lax.axis_index("corpus")
    twin = lax.axis_index("tensor")
    span = mine // group
    spot = lax.rem(mine, group)

    small = [(k_hbm, k_ref), (q_hbm, q_ref), (v_hbm, v_ref), (res_hbm, res_ref), (gain_hbm, gain_ref)]
    loads = [pltpu.make_async_copy(s, d, in_sem.at[i]) for i, (s, d) in enumerate(small)]
    pass_load = pltpu.make_async_copy(pass_hbm, pass_ref, in_sem.at[len(small)])
    for load in loads:
        load.start()
    w_loads = []
    for n in range(chunks):
        cols = pl.ds(n * chunk, chunk)
        w_loads.append(pltpu.make_async_copy(w_hbm.at[:, cols], w_ref.at[:, cols], w_sem.at[n]))
        w_loads[n].start()
    pass_load.start()

    def to(c, t):
        return dict(device_id=(c, t), device_id_type=pl.DeviceIdType.MESH)

    barrier = pltpu.get_barrier_semaphore()

    def greet(d, carry):
        pl.semaphore_signal(barrier, inc=1, **to(lax.rem(mine + d, corpus), twin))
        return carry

    lax.fori_loop(1, corpus, greet, 0)
    for d in range(1, tensor):
        pl.semaphore_signal(barrier, inc=1, **to(mine, lax.rem(twin + d, tensor)))

    row = lax.broadcasted_iota(jnp.int32, (rows, key_count), 0)
    col = lax.broadcasted_iota(jnp.int32, (rows, key_count), 1)
    picked = jnp.zeros((rows, key_count), jnp.bool_)
    allowed = jnp.zeros((rows, key_count), jnp.bool_)
    for b in range(query_count):
        length = lengths[b]
        picked = picked | ((row == b) & (col == b * SEQ + length - 1))
        allowed = allowed | ((row == b) & (col >= b * SEQ) & (col < b * SEQ + length))
    picker = jnp.where(picked, 1.0, 0.0).astype(BF16)
    allow = jnp.concatenate([jnp.where(allowed, 1.0, 0.0)] * per_kv, axis=0) > 0.5
    loads[0].wait()
    loads[1].wait()
    last_query = jnp.dot(picker, q_ref[...], preferred_element_type=F32)
    loads[2].wait()
    pieces = []
    for h in range(kv_heads):
        heads = slice(h * HEAD_DIM, (h + 1) * HEAD_DIM)
        stacked = jnp.concatenate(
            [last_query[:, (h * per_kv + g) * HEAD_DIM:(h * per_kv + g + 1) * HEAD_DIM]
             for g in range(per_kv)], axis=0).astype(BF16)
        logits = lax.dot_general(
            stacked, k_ref[:, heads], (((1,), (1,)), ((), ())), preferred_element_type=F32
        ) / math.sqrt(HEAD_DIM)
        logits = jnp.where(allow, logits, -1e30)
        highest = jnp.max(logits, axis=-1, keepdims=True)
        weights = jnp.where(allow, jnp.exp(logits - highest), 0.0)
        total = jnp.maximum(jnp.sum(weights, axis=-1, keepdims=True), 1.0)
        context = jnp.dot((weights / total).astype(BF16), v_ref[:, heads], preferred_element_type=F32)
        pieces += [context[g * rows:(g + 1) * rows] for g in range(per_kv)]
    context = jnp.concatenate(pieces, axis=1).astype(BF16)
    loads[3].wait()
    loads[4].wait()
    residual = jnp.dot(picker, res_ref[...], preferred_element_type=F32)

    pl.semaphore_wait(barrier, corpus - 1 + tensor - 1)

    sends = []
    for n in range(chunks):
        w_loads[n].wait()
        part[n, 0] = jnp.dot(context, w_ref[:, n * chunk:(n + 1) * chunk], preferred_element_type=F32)
        for d in range(1, tensor):
            send = pltpu.make_async_remote_copy(
                src_ref=part.at[n, 0], dst_ref=part.at[n, d],
                send_sem=part_send.at[n, d], recv_sem=part_recv.at[n, d],
                **to(mine, lax.rem(twin + d, tensor)))
            send.start()
            sends.append(send)
    scaled = []
    squares = 0.0
    for n in range(chunks):
        total = part[n, 0]
        for d in range(1, tensor):
            sends[n * (tensor - 1) + d - 1].wait_recv()
            total = total + part[n, d]
        cols = slice(n * chunk, (n + 1) * chunk)
        piece = (residual[:, cols] + total) * gain_ref[:, cols]
        squares = squares + jnp.sum(piece * piece, axis=1, keepdims=True)
        scaled.append(piece)
    magnitude = jnp.maximum(jnp.sqrt(squares), 1.0)
    per_share = chunks // tensor
    for n in range(chunks):
        inner = (n % per_share) * chunk
        gathered[n // per_share, mine, :, inner:inner + chunk] = (
            scaled[n] / magnitude)[:query_count].astype(BF16)

    def far(d, block):
        return pltpu.make_async_remote_copy(
            src_ref=gathered.at[twin, block], dst_ref=gathered.at[twin, block],
            send_sem=far_send.at[d], recv_sem=far_recv.at[d],
            **to(lax.rem(span + d, spans) * group + spot, twin))

    def near(d, g, block):
        return pltpu.make_async_remote_copy(
            src_ref=gathered.at[twin, block], dst_ref=gathered.at[twin, block],
            send_sem=near_send.at[d, g], recv_sem=near_recv.at[d, g],
            **to(span * group + lax.rem(spot + g, group), twin))

    def beside(d, g, t, owner, block):
        return pltpu.make_async_remote_copy(
            src_ref=gathered.at[owner, block], dst_ref=gathered.at[owner, block],
            send_sem=twin_send.at[d, g, t], recv_sem=twin_recv.at[d, g, t],
            **to(mine, lax.rem(twin + t, tensor)))

    def block_of(d, g):
        return lax.rem(span - d + spans, spans) * group + lax.rem(spot - g + group, group)

    def loop(low, high, body):
        def step(i, carry):
            body(i)
            return carry
        lax.fori_loop(low, high, step, 0)

    def start_far(d):
        far(d, mine).start()

    loop(1, spans, start_far)
    for g in range(1, group):
        near(0, g, mine).start()

    def relay(d):
        block = block_of(d, 0)
        far(d, block).wait_recv()
        for g in range(1, group):
            near(d, g, block).start()
        for t in range(1, tensor):
            beside(d, 0, t, twin, block).start()

    loop(1, spans, relay)

    def hand_over(d):
        for g in range(1, group):
            block = block_of(d, g)
            near(d, g, block).wait_recv()
            for t in range(1, tensor):
                beside(d, g, t, twin, block).start()

    loop(0, spans, hand_over)

    def take(d, g):
        for t in range(1, tensor):
            owner = lax.rem(twin - t + tensor, tensor)
            beside(d, g, t, owner, block_of(d, g)).wait_recv()

    def take_all(d):
        for g in range(group):
            take(d, g)

    for g in range(1, group):
        take(0, g)
    loop(1, spans, take_all)
    pass_load.wait()

    tile = 16 // query_count

    def assemble(i):
        for t in range(tensor):
            joined = jnp.concatenate(
                [gathered[t, i * tile + j].astype(F32) for j in range(tile)], axis=0)
            embed[pl.ds(pl.multiple_of(i * 16, 16), 16), t * share:(t + 1) * share] = joined.astype(BF16)

    loop(0, corpus // tile, assemble)
    scores = lax.dot_general(
        embed[...], pass_ref[...], (((1,), (1,)), ((), ())), preferred_element_type=F32
    ) * SCORE_SCALE
    scores_ref[...] = scores
    scores_out = pltpu.make_async_copy(scores_ref, scores_hbm, out_sem)
    scores_out.start()

    queries = scores.shape[0]
    padded = norm_ref.shape[1]
    peak = jnp.max(scores, axis=1, keepdims=True)
    total = jnp.sum(jnp.exp(scores - peak), axis=1, keepdims=True)
    lane = lax.broadcasted_iota(jnp.int32, (queries, 128), 1)
    both = jnp.where(lane == 0, peak, total)
    if padded > queries:
        both = jnp.concatenate([both, jnp.ones((padded - queries, 128), F32)], axis=0)
    pair_stat[0] = jnp.transpose(both)[:2]

    pair = [
        pltpu.make_async_remote_copy(
            src_ref=pair_stat.at[0], dst_ref=pair_stat.at[t],
            send_sem=pair_send.at[t], recv_sem=pair_recv.at[t],
            **to(mine, lax.rem(twin + t, tensor)))
        for t in range(1, tensor)
    ]
    for send in pair:
        send.start()
    for send in pair:
        send.wait_recv()

    def merge(stats):
        peaks, totals = stats[:, 0, :], stats[:, 1, :]
        high = jnp.max(peaks, axis=0, keepdims=True)
        return high, jnp.sum(totals * jnp.exp(peaks - high), axis=0, keepdims=True)

    high, total = merge(pair_stat[...])
    all_stat[mine] = jnp.concatenate([high, total], axis=0)

    def stat(d, block):
        return pltpu.make_async_remote_copy(
            src_ref=all_stat.at[block], dst_ref=all_stat.at[block],
            send_sem=stat_send.at[d], recv_sem=stat_recv.at[d],
            **to(lax.rem(mine + d, corpus), twin))

    loop(1, corpus, lambda d: stat(d, mine).start())
    for send in sends:
        send.wait_send()
    loop(1, spans, lambda d: far(d, mine).wait_send())

    def drain(d):
        for g in range(group):
            if g:
                near(d, g, block_of(d, 0)).wait_send()
            for t in range(1, tensor):
                beside(d, g, t, twin, block_of(d, g)).wait_send()

    for g in range(1, group):
        near(0, g, mine).wait_send()
        for t in range(1, tensor):
            beside(0, g, t, twin, block_of(0, g)).wait_send()
    loop(1, spans, drain)
    for send in pair:
        send.wait_send()
    scores_out.wait()
    loop(1, corpus, lambda d: stat(d, lax.rem(mine - d + corpus, corpus)).wait_recv())
    high, total = merge(all_stat[...])
    norm_ref[...] = high + jnp.log(total)
    loop(1, corpus, lambda d: stat(d, mine).wait_send())


def on_device(sizes, q_states, k_states, v_states, residual, out_weight, final_gain, passages, lengths):
    corpus, tensor, group, chunks = sizes
    query_count = lengths.shape[0]
    queries = query_count * corpus
    rows = -(-query_count // 8) * 8
    width = out_weight.shape[1]
    padded = -(-queries // 128) * 128
    spans = corpus // group
    local = passages.shape[0]
    hbm = pl.BlockSpec(memory_space=pl.ANY)
    dma = pltpu.SemaphoreType.DMA
    scores, norm = pl.pallas_call(
        functools.partial(kernel, sizes),
        out_shape=(
            jax.ShapeDtypeStruct((queries, local), F32),
            jax.ShapeDtypeStruct((1, padded), F32),
        ),
        in_specs=[pl.BlockSpec(memory_space=pltpu.SMEM)] + [hbm] * 7,
        out_specs=(hbm, pl.BlockSpec(memory_space=pltpu.VMEM)),
        scratch_shapes=[
            pltpu.VMEM(q_states.shape, BF16),
            pltpu.VMEM(k_states.shape, BF16),
            pltpu.VMEM(v_states.shape, BF16),
            pltpu.VMEM(residual.shape, BF16),
            pltpu.VMEM(out_weight.shape, BF16),
            pltpu.VMEM((1, width), F32),
            pltpu.VMEM(passages.shape, BF16),
            pltpu.VMEM((chunks, tensor, rows, width // chunks), F32),
            pltpu.VMEM((tensor, corpus, query_count, width // tensor), BF16),
            pltpu.VMEM((queries, width), BF16),
            pltpu.VMEM((queries, local), F32),
            pltpu.VMEM((tensor, 2, padded), F32),
            pltpu.VMEM((corpus, 2, padded), F32),
            dma((6,)), dma((chunks,)), dma,
            dma((chunks, tensor)), dma((chunks, tensor)),
            dma((spans,)), dma((spans,)),
            dma((spans, group)), dma((spans, group)),
            dma((spans, group, tensor)), dma((spans, group, tensor)),
            dma((tensor,)), dma((tensor,)),
            dma((corpus,)), dma((corpus,)),
        ],
        compiler_params=pltpu.CompilerParams(
            collective_id=0, has_side_effects=True, vmem_limit_bytes=60 * 1024 * 1024
        ),
    )(lengths, q_states, k_states, v_states, residual, out_weight, final_gain.reshape(1, -1), passages)
    return scores, norm[0, :queries]


def solution(mesh):
    corpus, tensor = mesh.shape["corpus"], mesh.shape["tensor"]
    group = GROUP if corpus % GROUP == 0 else 1
    sizes = (corpus, tensor, group, 4 * tensor)
    in_specs = (
        P("corpus", "tensor"),
        P("corpus", "tensor"),
        P("corpus", "tensor"),
        P("corpus", None),
        P("tensor", None),
        P(),
        P(("corpus", "tensor"), None),
        P("corpus"),
    )
    out_specs = (P(None, ("corpus", "tensor")), P())
    return jax.shard_map(
        functools.partial(on_device, sizes), mesh=mesh, in_specs=in_specs, out_specs=out_specs,
        check_vma=False,
    )
```
